32 devices in a mesh: tm: 4 (over x, core), anta: 4 (over z), antb: 2 (over y).
Axes of the slice: x: 2, y: 2, z: 4, core: 2. Of those that a mesh axis runs over, the one named last changes fastest.
Arguments:
- samples: bfloat16 [2, 512, 6144], P('antb', 'anta', 'tm'), may hold values from -6 to 6
Outputs:
- correlation: float32 [256, 2, 512, 2, 512], P('tm', None, 'anta', 'antb')
The draws below stay inside these ranges and needn't reach their ends.
All inputs are finite; a program needn't handle non-finite values.
Results may differ from the reference program's by a relative error of at most 0.0003.
Values may be sent and summed in bfloat16 or wider, within the bound.
A program may use at most 128 MiB of HBM per device.

```python
import math
import jax
import jax.numpy as jnp
from jax import lax

ANTENNA_COUNT = 512
POLARISATION_NUM = 2
LAG_TOTAL = 256
TIME = 6144


def block_levels(rng, extent, pieces, smallest, largest):
    gain, own = 1.0, jax.random.fold_in(rng, 6)
    for position, blocks in pieces:
        steps = jnp.exp(jax.random.uniform(jax.random.fold_in(own, position), (blocks,), jnp.float32, smallest / len(pieces), largest / len(pieces)))
        gain = gain * jnp.repeat(steps, extent[position] // blocks).reshape([-1 if axis == position else 1 for axis in range(len(extent))])
    return gain


def centred(own_key, shape, spread, most, cuts=(), kind=jnp.bfloat16):
    array = spread * jax.random.normal(own_key, shape, jnp.float32)
    if cuts:
        array = array * block_levels(own_key, shape, cuts, -0.22, 0.18)
    return jnp.clip(array, -most, most).astype(kind)


def setup_inputs(seed: int = 0) -> dict:
    key_of = jax.random.split(jax.random.key(seed), 2)
    samples = centred(key_of[0], (POLARISATION_NUM, ANTENNA_COUNT, TIME), 1.0, 6.0, ((0, 2), (1, 4), (2, 4)))
    return dict(samples=samples)


def reference(samples):
    flat_samples = samples.reshape(POLARISATION_NUM * ANTENNA_COUNT, TIME)
    padded = jnp.pad(flat_samples, ((0, 0), (0, LAG_TOTAL)))

    def one_lag(lag_index):
        shifted = lax.dynamic_slice_in_dim(padded, lag_index, TIME, 1)
        return jnp.dot(flat_samples, shifted.T, preferred_element_type=jnp.float32)
    lagged = lax.map(one_lag, jnp.arange(LAG_TOTAL, dtype=jnp.int32))
    return (lagged * (1.0 / math.sqrt(TIME))).reshape(LAG_TOTAL, POLARISATION_NUM, ANTENNA_COUNT, POLARISATION_NUM, ANTENNA_COUNT)
```

```python
import functools
import math

import jax
import jax.numpy as jnp
from jax import lax
from jax.experimental import pallas as pl
from jax.experimental.pallas import tpu as pltpu
from jax.sharding import PartitionSpec as P

LAG_TOTAL = 256
LANES = 128


def correlate_kernel(factor, stride, lags, cols_hbm, other_hbm, out_ref, rows, cols, hankel, sems):
    blocks, ring, height = cols_hbm.shape[:3]
    units = blocks * LANES
    window = stride * units
    step = pl.program_id(0)
    lag_start = lax.axis_index("tm") * lags

    def fill(entry):
        back = (lags - 1) + lag_start - entry
        shift = (back + stride - 1) // stride
        residue = shift * stride - back
        tile = rows[:, pl.ds(pl.multiple_of(residue * units, units), units)].astype(jnp.float32)
        rolled = pltpu.roll(tile, shift, 1)
        lane = lax.broadcasted_iota(jnp.int32, rolled.shape, 1)
        rolled = jnp.where(lane >= shift, rolled, 0.0)
        hankel[:, pl.ds(pl.multiple_of(entry * units, units), units)] = rolled.astype(jnp.bfloat16)

    def copies():
        anta, antb = lax.axis_index("anta"), lax.axis_index("antb")
        same = pl.ds(pl.multiple_of(antb * height, height), height)
        cross = pl.ds(pl.multiple_of((1 - antb) * height, height), height)
        for block in range(blocks):
            for r in range(stride):
                src = pl.ds(r * LANES, LANES)
                dst = pl.ds(r * units + block * LANES, LANES)
                yield cols_hbm.at[block, anta, :, src], rows.at[same, dst], sems.at[ring, block, r]
                yield other_hbm.at[block, :, src], rows.at[cross, dst], sems.at[ring + 1, block, r]
        for block in range(blocks):
            for r in range(stride):
                src = pl.ds(r * LANES, LANES)
                dst = pl.ds(r * units + block * LANES, LANES)
                for place in range(ring):
                    there = pl.ds(place * height, height)
                    yield cols_hbm.at[block, place, :, src], cols.at[there, dst], sems.at[place, block, r]

    @pl.when(step == 0)
    def _():
        for src, dst, sem in copies():
            pltpu.make_async_copy(src, dst, sem).start()
        for src, dst, sem in copies():
            pltpu.make_async_copy(src, dst, sem).wait()

        @pl.loop(0, stride)
        def _(index):
            fill(lags - 1 + index)

    @pl.when(step > 0)
    def _():
        fill(lags - 1 - step)

    offset = pl.multiple_of((lags - 1 - step) * units, units)
    lhs = hankel[:, pl.ds(offset, window)]
    res = lax.dot_general(lhs, cols[...], (((1,), (1,)), ((), ())), preferred_element_type=jnp.float32)
    res = res * factor
    pieces = res.shape[1] // LANES
    for piece in range(pieces):
        out_ref[0, pl.ds(piece, res.shape[0], stride=pieces), :] = res[:, piece * LANES:(piece + 1) * LANES]


def correlate(cols, other, lags, factor):
    blocks, ring, height, width = cols.shape
    row_count, col_count = 2 * height, ring * height
    stride = width // LANES
    window = blocks * width
    pieces = col_count // LANES
    return pl.pallas_call(
        functools.partial(correlate_kernel, factor, stride, lags),
        grid=(lags,),
        out_shape=jax.ShapeDtypeStruct((lags, row_count * pieces, LANES), jnp.float32),
        in_specs=[pl.BlockSpec(memory_space=pl.ANY)] * 2,
        out_specs=pl.BlockSpec((1, row_count * pieces, LANES), lambda i: (i, 0, 0)),
        scratch_shapes=[
            pltpu.VMEM((row_count, window), jnp.bfloat16),
            pltpu.VMEM((col_count, window), jnp.bfloat16),
            pltpu.VMEM((row_count, (lags - 1 + stride) * blocks * LANES), jnp.bfloat16),
            pltpu.SemaphoreType.DMA((ring + 2, blocks, stride)),
        ],
        compiler_params=pltpu.CompilerParams(vmem_limit_bytes=60 * 1024 * 1024),
    )(cols, other)


def gather_kernel(own, cols, other, local_sem, ring_send, ring_recv, near_send, near_recv,
                  far_send, far_recv, pol_send, pol_recv):
    tm, anta, antb = (lax.axis_index(name) for name in ("tm", "anta", "antb"))
    blocks, ring = cols.shape[:2]
    height = own.shape[0]
    half = height // 2
    far = lax.rem(tm + blocks // 2, blocks)
    near = tm + 1 - 2 * lax.rem(tm, 2)
    right, left = lax.rem(anta + 1, ring), lax.rem(anta + ring - 1, ring)
    to_far, to_near, to_pol = {"tm": far}, {"tm": near}, {"antb": 1 - antb}
    sides = ({"anta": right}, {"anta": left})

    barrier = pltpu.get_barrier_semaphore()
    for target in (to_far, to_near, to_pol) + sides:
        pl.semaphore_signal(barrier, inc=1, device_id=target, device_id_type=pl.DeviceIdType.MESH)
    pl.semaphore_wait(barrier, 5)

    started = []

    def send(src, dst, send_sem, recv_sem, target):
        copy = pltpu.make_async_remote_copy(
            src_ref=src, dst_ref=dst, send_sem=send_sem, recv_sem=recv_sem,
            device_id=target, device_id_type=pl.DeviceIdType.MESH)
        copy.start()
        started.append(copy)
        return copy

    times = (tm, far)
    last = ring // 2
    hops, nears = {}, []

    def part(side, hop):
        if hop < last:
            return pl.ds(0, height)
        return pl.ds(side * half, half)

    def pass_on(stream, side, hop, src=None):
        place = lax.rem(anta + (ring - hop + 1 if side == 0 else hop - 1), ring)
        rows = part(side, hop)
        slot = cols.at[times[stream], place, rows]
        src = slot if src is None else src.at[rows]
        hops[stream, side, hop] = send(src, slot, ring_send.at[stream, side, hop - 1],
                                       ring_recv.at[stream, side, hop - 1], sides[side])

    def hand(stream, offset, src=None):
        slot = cols.at[times[stream], lax.rem(anta + offset, ring)]
        nears.append(send(slot if src is None else src, slot, near_send.at[stream, offset],
                          near_recv.at[stream, offset], to_near))

    def arrive(stream, hop):
        for side in range(2):
            hops[stream, side, hop].wait_recv()
            if hop < last:
                pass_on(stream, side, hop + 1)
                hand(stream, ring - hop if side == 0 else hop)
        if hop == last:
            hand(stream, last)

    slot = cols.at[tm, anta]
    first = send(own, slot, far_send.at[0], far_recv.at[0], to_far)
    pol = send(own, other.at[tm], pol_send, pol_recv, to_pol)
    for side in range(2):
        pass_on(0, side, 1, own)
    hand(0, 0, own)
    keep = pltpu.make_async_copy(own, slot, local_sem)
    keep.start()

    first.wait_recv()
    for side in range(2):
        pass_on(1, side, 1)
    hand(1, 0)
    pol.wait_recv()
    second = send(other.at[tm], other.at[tm], far_send.at[1], far_recv.at[1], to_far)
    nears.append(send(other.at[tm], other.at[tm], near_send.at[0, ring], near_recv.at[0, ring], to_near))
    for hop in range(1, last + 1):
        arrive(0, hop)
        if hop == 1:
            second.wait_recv()
            nears.append(send(other.at[far], other.at[far], near_send.at[1, ring],
                              near_recv.at[1, ring], to_near))
        arrive(1, hop)
    for copy in nears:
        copy.wait_recv()
    for copy in started:
        copy.wait_send()
    keep.wait()


def gather(own):
    blocks, ring = lax.axis_size("tm"), lax.axis_size("anta")
    dma = pltpu.SemaphoreType.DMA
    return pl.pallas_call(
        gather_kernel,
        out_shape=[
            jax.ShapeDtypeStruct((blocks, ring) + own.shape, own.dtype),
            jax.ShapeDtypeStruct((blocks,) + own.shape, own.dtype),
        ],
        in_specs=[pl.BlockSpec(memory_space=pltpu.VMEM)],
        out_specs=[pl.BlockSpec(memory_space=pl.ANY)] * 2,
        scratch_shapes=[
            dma, dma((2, 2, ring // 2)), dma((2, 2, ring // 2)), dma((2, ring + 1)), dma((2, ring + 1)),
            dma((2,)), dma((2,)), dma, dma,
        ],
        compiler_params=pltpu.CompilerParams(collective_id=0, has_side_effects=True),
    )(own)


def per_device(samples):
    antennas, width = samples.shape[1:]
    blocks = lax.axis_size("tm")
    lags = LAG_TOTAL // blocks
    own = samples[0].reshape(antennas, LANES, width // LANES).transpose(0, 2, 1).reshape(antennas, width)
    cols, other = gather(own)
    factor = 1.0 / math.sqrt(width * blocks)
    out = correlate(cols, other, lags, factor)
    return out.reshape(lags, -1, antennas, 1, cols.shape[1] * antennas)


def solution(mesh):
    return jax.shard_map(
        per_device,
        mesh=mesh,
        in_specs=(P("antb", "anta", "tm"),),
        out_specs=P("tm", None, "anta", "antb", None),
        check_vma=False,
    )
```
